256 devices in a mesh: chain: 128 (over y_lo, x, z, core), shard: 2 (over y_hi).
Axes of the slice: x: 4, y: 4 (y_hi: 2, y_lo: 2; y = y_hi * 2 + y_lo), z: 8, core: 2. Of those that a mesh axis runs over, the one named last changes fastest.
Arguments:
- w_pair: bfloat16 [128, 2, 256, 4096], P('chain', None, 'shard'), may hold values from -6 to 6
- w_down: bfloat16 [128, 256, 4096], P('chain', 'shard'), may hold values from -6 to 6
- tokens: bfloat16 [128, 512, 4096], P('chain', 'shard'), may hold values from -6 to 6
- cotangent: bfloat16 [128, 512, 4096], P('chain', 'shard'), may hold values from -6 to 6
- seq_ids: int32 [128, 512], P('chain', 'shard'), may hold values from 0 to 7, never falling along the last dimension, each value on 1 to 128 neighbouring positions
- msg_left: bfloat16 [128, 2, 256, 4096], P('chain', None, 'shard'), may hold values from -9 to 9
- msg_right: bfloat16 [128, 2, 256, 4096], P('chain', None, 'shard'), may hold values from -9 to 9
- count_left: int32 [128], P('chain'), may hold values from 0 to 5, as said below
- count_right: int32 [128], P('chain'), may hold values from 0 to 5, as said below
Outputs:
- new_pair: bfloat16 [128, 2, 256, 4096], P('chain', None, 'shard')
The draws below stay inside these ranges and needn't reach their ends.
Inputs may be any that keep to these rules, and one draw needn't show every extreme that they name: count_left of worker w is at most min(w, 5); some worker at least 5 from both ends of the chain has count_left equal to 5. count_right of worker w is at most min(127 - w, 5); the same worker has count_right equal to 5.
All inputs are finite; a program needn't handle non-finite values.
Results may differ from the reference program's by a relative error of at most 0.0053.
Values may be sent and summed in bfloat16 or wider, within the bound.
A program may use at most 128 MiB of HBM per device.

```python
import math
import jax
import jax.numpy as jnp
import numpy as np
from jax import lax

D = 4096
SEQS = 8
H = 256
TOKW = 512
MAXLEN = 128
WORKERS = 128


def forced_worker(key):
    return jax.random.randint(jax.random.fold_in(key, 7), (), 5, WORKERS - 5, dtype=jnp.int32)


def capped_counts(key, salt, limits):
    raw_counts = jax.random.randint(jax.random.fold_in(key, salt), (WORKERS,), 0, 6, dtype=jnp.int32)
    worker_index = jnp.arange(WORKERS, dtype=jnp.int32)
    capped = jnp.minimum(raw_counts, jnp.minimum(limits, 5))
    return jnp.where(worker_index == forced_worker(key), 5, capped).astype(jnp.int32)


def draw_count_left(key, part):
    worker_index = jnp.arange(WORKERS, dtype=jnp.int32)
    return capped_counts(key, 11, worker_index)


def draw_count_right(key, part):
    worker_index = jnp.arange(WORKERS, dtype=jnp.int32)
    return capped_counts(key, 13, WORKERS - 1 - worker_index)


def block_scale(rng, dims, pieces, smallest, top_value):
    def one(position, blocks):
        draws = jax.random.uniform(jax.random.fold_in(jax.random.fold_in(rng, 6), position), (blocks,), jnp.float32, smallest / len(pieces), top_value / len(pieces))
        return jnp.repeat(jnp.exp(draws), dims[position] // blocks).reshape((-1,) + (1,) * (len(dims) - position - 1))

    factor_of = one(*pieces[0])
    for cut in pieces[1:]:
        factor_of = factor_of * one(*cut)
    return factor_of


def length_profile(number_of, total, bound, lean):
    weights = [(1 << 20) // math.isqrt(grade ** lean) + 1 for grade in range(2, number_of + 1)]
    surplus, holding = total - bound - (number_of - 1), [1] * (number_of - 1)
    while surplus > 0:
        free = [i for i in range(number_of - 1) if holding[i] < bound]
        whole, remaining = sum([weights[i] for i in free]), surplus
        for i in free:
            extra = min(bound - holding[i], max(1, remaining * weights[i] // whole), surplus)
            holding[i] = holding[i] + extra
            surplus = surplus - extra
    return np.array([bound] + holding)


def ragged(rng, amount, total, bound, lean):
    if amount == 2:
        one = jax.random.randint(rng, (), max(1, total - bound), min(bound, total - 1) + 1)
        return jnp.stack([one, total - one])
    tallies = jnp.asarray(length_profile(amount, total, bound, lean), jnp.int32)
    couples = (amount - 1) // 2
    source_of, sink = tallies[1:1 + 2 * couples:2], tallies[2:2 + 2 * couples:2]
    margin = jnp.minimum(source_of - 1, bound - sink)
    moved = jax.random.randint(jax.random.fold_in(rng, 1), (couples,), 0, 1 << 20) % (margin + 1)
    tallies = tallies.at[1:1 + 2 * couples:2].set(source_of - moved).at[2:2 + 2 * couples:2].set(sink + moved)
    return tallies[jax.random.permutation(jax.random.fold_in(rng, 2), amount)]


def normal_values(key, dims, width, reach, split=(), kind=jnp.bfloat16):
    entries = jax.random.normal(key, dims, jnp.float32) * width
    if len(split) > 0:
        entries = block_scale(key, dims, split, -0.22, 0.18) * entries
    return jnp.clip(entries, min=-reach, max=reach).astype(kind)


def setup_inputs(seed: int = 0) -> dict:
    key_list = jax.random.split(jax.random.key(seed), 10)
    w_pair = normal_values(key_list[0], (WORKERS, 2, H, D), 1.0, 6.0, ((0, 128), (2, 2)))
    w_down = normal_values(key_list[1], (WORKERS, H, D), 1.0, 6.0, ((0, 128), (1, 2)))
    tokens = normal_values(key_list[2], (WORKERS, TOKW, D), 1.0, 6.0, ((0, 128), (1, 2)))
    cotangent = normal_values(key_list[3], (WORKERS, TOKW, D), 1.0, 6.0, ((0, 128), (1, 2)))
    seq_ids = jax.vmap(lambda own: jnp.searchsorted(jnp.cumsum(ragged(own, SEQS, TOKW, MAXLEN, 1)), jnp.arange(TOKW), side="right"))(jax.random.split(key_list[4], WORKERS)).reshape((WORKERS, TOKW)).astype(jnp.int32)
    msg_left = normal_values(key_list[5], (WORKERS, 2, H, D), 1.5, 9.0, ((0, 128), (2, 2)))
    msg_right = normal_values(key_list[6], (WORKERS, 2, H, D), 1.5, 9.0, ((0, 128), (2, 2)))
    count_left = draw_count_left(jax.random.fold_in(key_list[9], 71), 0)
    count_right = draw_count_right(jax.random.fold_in(key_list[9], 71), 0)
    return {"w_pair": w_pair, "w_down": w_down, "tokens": tokens, "cotangent": cotangent, "seq_ids": seq_ids, "msg_left": msg_left, "msg_right": msg_right, "count_left": count_left, "count_right": count_right}


learn_rate = 1.0


def worker_half(packed):
    w_pair_one, w_down_one, tokens_one, cotangent_one, seq_one = packed
    width_scale = D ** -0.5
    gate_pre = jnp.dot(tokens_one, w_pair_one[0].T, preferred_element_type=jnp.float32) * width_scale
    up_pre = jnp.dot(tokens_one, w_pair_one[1].T, preferred_element_type=jnp.float32) * width_scale
    one_hot = (seq_one[:, None] == jnp.arange(SEQS, dtype=jnp.int32)[None, :]).astype(jnp.float32)
    seq_count = jnp.sum(one_hot, axis=0)
    seq_len = jnp.sum(one_hot * seq_count[None, :], axis=1)
    tok_weight = (TOKW / SEQS) / seq_len
    scaled_cot = (tok_weight[:, None] * cotangent_one.astype(jnp.float32)).astype(jnp.bfloat16)
    grad_hidden = jnp.dot(scaled_cot, w_down_one.T, preferred_element_type=jnp.float32) * width_scale
    sigmoid_gate = jax.nn.sigmoid(gate_pre)
    grad_gate = (grad_hidden * up_pre * sigmoid_gate * (1.0 + gate_pre * (1.0 - sigmoid_gate))).astype(jnp.bfloat16)
    grad_up = (grad_hidden * gate_pre * sigmoid_gate).astype(jnp.bfloat16)
    batch_scale = TOKW ** -0.5
    gate_weight_grad = jnp.dot(grad_gate.T, tokens_one, preferred_element_type=jnp.float32) * batch_scale
    up_weight_grad = jnp.dot(grad_up.T, tokens_one, preferred_element_type=jnp.float32) * batch_scale
    return w_pair_one.astype(jnp.float32) - learn_rate * jnp.stack([gate_weight_grad, up_weight_grad])


def reference(w_pair, w_down, tokens, cotangent, seq_ids, msg_left, msg_right, count_left, count_right):
    half_step = lax.map(worker_half, (w_pair, w_down, tokens, cotangent, seq_ids))
    send_right = (half_step + msg_left.astype(jnp.float32)).astype(jnp.bfloat16)
    send_left = (half_step + msg_right.astype(jnp.float32)).astype(jnp.bfloat16)
    zero_msg = jnp.zeros_like(send_right[:1])
    recv_left = jnp.concatenate([zero_msg, send_right[:-1]], axis=0)
    recv_right = jnp.concatenate([send_left[1:], zero_msg], axis=0)
    zero_count = jnp.zeros((1,), jnp.int32)
    cnt_left = jnp.concatenate([zero_count, (count_left[:-1] + 1).astype(jnp.int32)], axis=0)
    cnt_right = jnp.concatenate([(count_right[1:] + 1).astype(jnp.int32), zero_count], axis=0)
    total_count = (1 + cnt_left + cnt_right).astype(jnp.float32)
    summed = half_step + recv_left.astype(jnp.float32) + recv_right.astype(jnp.float32)
    return (summed / total_count[:, None, None, None]).astype(jnp.bfloat16)
```

```python
import functools

import jax
import jax.numpy as jnp
from jax import lax
from jax.experimental import pallas as pl
from jax.experimental.pallas import tpu as pltpu
from jax.sharding import PartitionSpec as P

MESH = pl.DeviceIdType.MESH
F32 = jnp.float32
BF16 = jnp.bfloat16
learn_rate = 1.0
SEQS = 8

CHUNKS = ((0, 32), (32, 32), (64, 32), (96, 16), (112, 16))
TILE = 512


def dot_nt(a, b):
    return lax.dot_general(a, b, (((1,), (1,)), ((), ())), preferred_element_type=F32)


def gate_factors(pre, hidden):
    gate, up = pre[:hidden], pre[hidden:]
    sig = jax.nn.sigmoid(gate)
    return up * sig * (1.0 + gate * (1.0 - sig)), gate * sig


def kernel(
    workers,
    w_pair,
    w_down,
    tokens,
    cotangent,
    seq_ids,
    msg_left,
    msg_right,
    count_left,
    count_right,
    out,
    wp,
    wd,
    tok,
    cot,
    ids,
    ml,
    mr,
    cl,
    cr,
    tok_p,
    wd_p,
    ids_p,
    gh_out,
    gh_p,
    fac_gate,
    fac_up,
    lhs,
    weight,
    half,
    send_r,
    send_l,
    recv_l,
    recv_r,
    cnt_r_out,
    cnt_l_out,
    cnt_l,
    cnt_r,
    new,
    load_sem,
    out_sem,
    y_send,
    y_recv,
    wd_send,
    wd_recv,
    gh_send,
    gh_recv,
    r_send,
    r_recv,
    l_send,
    l_recv,
):
    me, side = lax.axis_index("chain"), lax.axis_index("shard")
    partner = (me, 1 - side)
    last = workers - 1
    right, left = ((me + 1) % workers, side), ((me + last) % workers, side)
    has_left, has_right = me > 0, me < last
    rows, width = tok.shape
    hidden = wd.shape[0]
    width_scale = width**-0.5
    batch_scale = (2 * rows) ** -0.5
    n = len(CHUNKS)
    tiles = width // TILE

    def remote(src, dst, send, recv, device):
        return pltpu.make_async_remote_copy(
            src_ref=src, dst_ref=dst, send_sem=send, recv_sem=recv, device_id=device, device_id_type=MESH
        )

    def cols(j):
        return pl.ds(pl.multiple_of(j * TILE, TILE), TILE)

    barrier = pltpu.get_barrier_semaphore()
    pl.semaphore_signal(barrier, inc=1, device_id=partner, device_id_type=MESH)

    @pl.when(has_left)
    def _():
        pl.semaphore_signal(barrier, inc=1, device_id=left, device_id_type=MESH)

    @pl.when(has_right)
    def _():
        pl.semaphore_signal(barrier, inc=1, device_id=right, device_id_type=MESH)

    loads = [
        pltpu.make_async_copy(src, dst, load_sem.at[k])
        for k, (src, dst) in enumerate(
            (
                (tokens.at[0], tok),
                (w_pair.at[0], wp),
                (cotangent.at[0], cot),
                (w_down.at[0], wd),
                (seq_ids, ids),
                (msg_left.at[0], ml),
                (msg_right.at[0], mr),
                (count_left, cl),
                (count_right, cr),
            )
        )
    ]
    for load in loads:
        load.start()

    pl.semaphore_wait(barrier, 1 + has_left.astype(jnp.int32) + has_right.astype(jnp.int32))

    ids_copy = remote(seq_ids, ids_p, y_send.at[0], y_recv.at[0], partner)
    tok_copy = remote(tokens.at[0], tok_p, y_send.at[1], y_recv.at[1], partner)
    wd_copies = [
        remote(
            w_down.at[0, pl.ds(r0, r)], wd_p.at[pl.ds(r0, r)], wd_send.at[c], wd_recv.at[c], partner
        )
        for c, (r0, r) in enumerate(CHUNKS)
    ]
    gh_copies = [
        remote(gh_out.at[pl.ds(r0, r)], gh_p.at[pl.ds(r0, r)], gh_send.at[c], gh_recv.at[c], partner)
        for c, (r0, r) in enumerate(CHUNKS)
    ]
    r_copies = [
        remote(
            send_r.at[:, pl.ds(r0, r)], recv_l.at[:, pl.ds(r0, r)], r_send.at[c], r_recv.at[c], right
        )
        for c, (r0, r) in enumerate(CHUNKS)
    ] + [remote(cnt_r_out, cnt_l, r_send.at[n], r_recv.at[n], right)]
    l_copies = [
        remote(
            send_l.at[:, pl.ds(r0, r)], recv_r.at[:, pl.ds(r0, r)], l_send.at[c], l_recv.at[c], left
        )
        for c, (r0, r) in enumerate(CHUNKS)
    ] + [remote(cnt_l_out, cnt_r, l_send.at[n], l_recv.at[n], left)]
    out_copies = [
        pltpu.make_async_copy(
            new.at[:, pl.ds(r0, r)], out.at[0, :, pl.ds(r0, r)], out_sem.at[c]
        )
        for c, (r0, r) in enumerate(CHUNKS)
    ]

    def send_chain(c):
        @pl.when(has_right)
        def _():
            r_copies[c].start()

        @pl.when(has_left)
        def _():
            l_copies[c].start()

    ids_copy.start()
    wd_copies[0].start()
    tok_copy.start()

    @pl.when(jnp.logical_not(has_left))
    def _():
        recv_l[...] = jnp.zeros_like(recv_l)
        cnt_l[...] = jnp.zeros_like(cnt_l)

    @pl.when(jnp.logical_not(has_right))
    def _():
        recv_r[...] = jnp.zeros_like(recv_r)
        cnt_r[...] = jnp.zeros_like(cnt_r)

    loads[0].wait()
    loads[1].wait()
    w_all = wp[...].reshape(2 * hidden, width)
    gate_own, up_own = gate_factors(dot_nt(w_all, tok[...]) * width_scale, hidden)

    loads[4].wait()
    ids_copy.wait_recv()
    own_row = ids[...]
    shape = (rows, rows)
    diag = lax.broadcasted_iota(jnp.int32, shape, 0) == lax.broadcasted_iota(jnp.int32, shape, 1)
    own_col = jnp.sum(jnp.where(diag, own_row, 0), axis=1, keepdims=True)
    peer_col = jnp.sum(jnp.where(diag, ids_p[...], 0), axis=1, keepdims=True)
    seq_len = jnp.sum((own_col == own_row).astype(F32), axis=0, keepdims=True) + jnp.sum(
        (peer_col == own_row).astype(F32), axis=0, keepdims=True
    )
    weight[...] = (2 * rows / SEQS) / seq_len * width_scale

    loads[2].wait()
    loads[3].wait()
    gh_own = dot_nt(wd[...], cot[...]) * weight[...]
    lhs[:hidden] = (gh_own * gate_own).astype(BF16)
    lhs[hidden:] = (gh_own * up_own).astype(BF16)

    def own_tile(j, carry):
        part = jnp.dot(lhs[...], tok[:, cols(j)], preferred_element_type=F32)
        part = part.reshape(2, hidden, TILE) * (learn_rate * batch_scale)
        half[:, :, cols(j)] = wp[:, :, cols(j)].astype(F32) - part
        return carry

    lax.fori_loop(0, tiles, own_tile, 0)

    def partner_grad_hidden(c):
        r0, r = CHUNKS[c]
        wd_copies[c].wait_recv()
        gh = dot_nt(wd_p[r0 : r0 + r], cot[...]) * weight[...]
        gh_out[r0 : r0 + r] = gh.astype(BF16)
        gh_copies[c].start()

    def finish_rows(c):
        r0, r = CHUNKS[c]
        gh_copies[c].wait_recv()
        gh = gh_p[r0 : r0 + r].astype(F32)
        both = jnp.concatenate(
            [gh * fac_gate[r0 : r0 + r], gh * fac_up[r0 : r0 + r]], axis=0
        ).astype(BF16)

        def tile(j, carry):
            part = jnp.dot(both, tok_p[:, cols(j)], preferred_element_type=F32)
            part = part.reshape(2, r, TILE) * (learn_rate * batch_scale)
            step = half[:, r0 : r0 + r, cols(j)] - part
            half[:, r0 : r0 + r, cols(j)] = step
            send_r[:, r0 : r0 + r, cols(j)] = (
                step + ml[:, r0 : r0 + r, cols(j)].astype(F32)
            ).astype(BF16)
            send_l[:, r0 : r0 + r, cols(j)] = (
                step + mr[:, r0 : r0 + r, cols(j)].astype(F32)
            ).astype(BF16)
            return carry

        lax.fori_loop(0, tiles, tile, 0)
        send_chain(c)

    partner_grad_hidden(0)
    for c in range(1, min(3, n)):
        wd_copies[c].start()

    for k in (5, 6, 7, 8):
        loads[k].wait()
    cnt_r_out[...] = jnp.full(cnt_r_out.shape, 1 + cl[0], jnp.int32)
    cnt_l_out[...] = jnp.full(cnt_l_out.shape, 1 + cr[0], jnp.int32)
    send_chain(n)

    tok_copy.wait_recv()
    gate_peer, up_peer = gate_factors(dot_nt(w_all, tok_p[...]) * width_scale, hidden)
    fac_gate[...] = gate_peer
    fac_up[...] = up_peer
    finish_rows(0)
    for c in range(1, n):
        partner_grad_hidden(c)
        if c + 2 < n:
            wd_copies[c + 2].start()
        if c >= 2:
            finish_rows(c - 1)
    finish_rows(n - 1)

    @pl.when(has_left)
    def _():
        r_copies[n].wait_recv()

    @pl.when(has_right)
    def _():
        l_copies[n].wait_recv()

    inverse = 1.0 / (1.0 + cnt_l[...].astype(F32) + cnt_r[...].astype(F32))

    for c, (r0, r) in enumerate(CHUNKS):

        @pl.when(has_left)
        def _(c=c):
            r_copies[c].wait_recv()

        @pl.when(has_right)
        def _(c=c):
            l_copies[c].wait_recv()

        def tile(j, carry, r0=r0, r=r):
            total = (
                half[:, r0 : r0 + r, cols(j)]
                + recv_l[:, r0 : r0 + r, cols(j)].astype(F32)
                + recv_r[:, r0 : r0 + r, cols(j)].astype(F32)
            )
            new[:, r0 : r0 + r, cols(j)] = (total * inverse.reshape(1, 1, TILE)).astype(BF16)
            return carry

        lax.fori_loop(0, tiles, tile, 0)
        out_copies[c].start()

    ids_copy.wait_send()
    tok_copy.wait_send()
    for c in range(n):
        wd_copies[c].wait_send()
        gh_copies[c].wait_send()
    for c in range(n + 1):

        @pl.when(has_right)
        def _(c=c):
            r_copies[c].wait_send()

        @pl.when(has_left)
        def _(c=c):
            l_copies[c].wait_send()

    for copy in out_copies:
        copy.wait()


def body(w_pair, w_down, tokens, cotangent, seq_ids, msg_left, msg_right, count_left, count_right):
    workers = lax.axis_size("chain")
    pair = w_pair.shape[1:]
    hidden, width = pair[1:]
    rows = tokens.shape[1]
    n = len(CHUNKS)
    any_space = pl.BlockSpec(memory_space=pltpu.HBM)
    vm, dma = pltpu.VMEM, pltpu.SemaphoreType.DMA
    return pl.pallas_call(
        functools.partial(kernel, workers),
        out_shape=jax.ShapeDtypeStruct(w_pair.shape, BF16),
        in_specs=[any_space] * 9,
        out_specs=any_space,
        scratch_shapes=[
            vm(pair, BF16),
            vm((hidden, width), BF16),
            vm((rows, width), BF16),
            vm((rows, width), BF16),
            vm((1, rows), jnp.int32),
            vm(pair, BF16),
            vm(pair, BF16),
            pltpu.SMEM((1,), jnp.int32),
            pltpu.SMEM((1,), jnp.int32),
            vm((rows, width), BF16),
            vm((hidden, width), BF16),
            vm((1, rows), jnp.int32),
            vm((hidden, rows), BF16),
            vm((hidden, rows), BF16),
            vm((hidden, rows), F32),
            vm((hidden, rows), F32),
            vm((2 * hidden, rows), BF16),
            vm((1, rows), F32),
            vm(pair, F32),
            vm(pair, BF16),
            vm(pair, BF16),
            vm(pair, BF16),
            vm(pair, BF16),
            vm((1, TILE), jnp.int32),
            vm((1, TILE), jnp.int32),
            vm((1, TILE), jnp.int32),
            vm((1, TILE), jnp.int32),
            vm(pair, BF16),
            dma((9,)),
            dma((n,)),
            dma((2,)),
            dma((2,)),
            dma((n,)),
            dma((n,)),
            dma((n,)),
            dma((n,)),
            dma((n + 1,)),
            dma((n + 1,)),
            dma((n + 1,)),
            dma((n + 1,)),
        ],
        compiler_params=pltpu.CompilerParams(
            collective_id=0, has_side_effects=True, vmem_limit_bytes=60 * 1024 * 1024
        ),
    )(w_pair, w_down, tokens, cotangent, seq_ids, msg_left, msg_right, count_left, count_right)


def solution(mesh):
    return jax.shard_map(
        body,
        mesh=mesh,
        in_specs=(
            P("chain", None, "shard", None),
            P("chain", "shard", None),
            P("chain", "shard", None),
            P("chain", "shard", None),
            P("chain", "shard"),
            P("chain", None, "shard", None),
            P("chain", None, "shard", None),
            P("chain"),
            P("chain"),
        ),
        out_specs=P("chain", None, "shard", None),
        check_vma=False,
    )
```

```python
import functools

import jax
import jax.numpy as jnp
from jax import lax
from jax.experimental import pallas as pl
from jax.experimental.pallas import tpu as pltpu
from jax.sharding import PartitionSpec as P

MESH = pl.DeviceIdType.MESH
F32 = jnp.float32
BF16 = jnp.bfloat16
learn_rate = 1.0
SEQS = 8

CHUNKS = ((0, 32), (32, 32), (64, 32), (96, 16), (112, 16))
TILE = 512

X, Z = 4, 8
PIECE = 16
RELAYS = 12


def dot_nt(a, b):
    return lax.dot_general(a, b, (((1,), (1,)), ((), ())), preferred_element_type=F32)


def gate_factors(pre, hidden):
    gate, up = pre[:hidden], pre[hidden:]
    sig = jax.nn.sigmoid(gate)
    return up * sig * (1.0 + gate * (1.0 - sig)), gate * sig


def kernel(
    workers,
    w_pair,
    w_down,
    tokens,
    cotangent,
    seq_ids,
    msg_left,
    msg_right,
    count_left,
    count_right,
    out,
    wp,
    wd,
    tok,
    cot,
    ids,
    ml,
    mr,
    cl,
    cr,
    tok_p,
    wd_p,
    ids_p,
    gh_out,
    gh_p,
    fac_gate,
    fac_up,
    lhs,
    weight,
    half,
    send_r,
    send_l,
    recv_l,
    recv_r,
    cnt_r_out,
    cnt_l_out,
    cnt_l,
    cnt_r,
    load_sem,
    y_send,
    y_recv,
    wd_send,
    wd_recv,
    gh_send,
    gh_recv,
    r_send,
    r_recv,
    l_send,
    l_recv,
    relay_buf,
    relay_send,
    relay_recv,
):
    me, side = lax.axis_index("chain"), lax.axis_index("shard")
    partner = (me, 1 - side)
    last = workers - 1
    right, left = ((me + 1) % workers, side), ((me + last) % workers, side)
    has_left, has_right = me > 0, me < last
    rows, width = tok.shape
    hidden = wd.shape[0]
    width_scale = width**-0.5
    batch_scale = (2 * rows) ** -0.5
    n = len(CHUNKS)
    tiles = width // TILE

    def remote(src, dst, send, recv, device):
        return pltpu.make_async_remote_copy(
            src_ref=src, dst_ref=dst, send_sem=send, recv_sem=recv, device_id=device, device_id_type=MESH
        )

    def cols(j):
        return pl.ds(pl.multiple_of(j * TILE, TILE), TILE)

    edge_r, edge_l = workers // 2 - 1, workers // 2
    x, z, core, upper = (me // (2 * Z)) % X, (me // 2) % Z, me % 2, me >= edge_l

    def relay_right(p):
        return (edge_l + ((X - 1 - p % X) * Z + (Z - 1 + p // X) % Z) * 2 + 1, side)

    def relay_left(p):
        return (((p % X) * Z + (Z - p // X) % Z) * 2, side)

    on_right = upper & (core == 1) & ((z + 1) % Z < RELAYS // X)
    on_left = jnp.logical_not(upper) & (core == 0) & ((Z - z) % Z < RELAYS // X)
    piece = jnp.where(upper, (z + 1) % Z * X + X - 1 - x, (Z - z) % Z * X + x)
    piece = jnp.where(on_right | on_left, piece, 0)
    piece_rows = pl.ds(pl.multiple_of(piece // 2 * PIECE, PIECE), PIECE)
    piece_chunk = sum((piece // 2 * PIECE >= r0).astype(jnp.int32) for r0, _ in CHUNKS) - 1
    relayed = [r0 + r <= RELAYS // 2 * PIECE for r0, r in CHUNKS] + [False]

    barrier = pltpu.get_barrier_semaphore()
    pl.semaphore_signal(barrier, inc=1, device_id=partner, device_id_type=MESH)

    @pl.when(has_left)
    def _():
        pl.semaphore_signal(barrier, inc=1, device_id=left, device_id_type=MESH)

    @pl.when(has_right)
    def _():
        pl.semaphore_signal(barrier, inc=1, device_id=right, device_id_type=MESH)

    @pl.when(on_right)
    def _():
        pl.semaphore_signal(barrier, inc=1, device_id=(edge_r, side), device_id_type=MESH)

    @pl.when(on_left)
    def _():
        pl.semaphore_signal(barrier, inc=1, device_id=(edge_l, side), device_id_type=MESH)

    @pl.when(me == edge_l)
    def _():
        for p in range(RELAYS):
            pl.semaphore_signal(barrier, inc=1, device_id=relay_right(p), device_id_type=MESH)

    @pl.when(me == edge_r)
    def _():
        for p in range(RELAYS):
            pl.semaphore_signal(barrier, inc=1, device_id=relay_left(p), device_id_type=MESH)

    loads = [
        pltpu.make_async_copy(src, dst, load_sem.at[k])
        for k, (src, dst) in enumerate(
            (
                (tokens.at[0], tok),
                (w_pair.at[0], wp),
                (cotangent.at[0], cot),
                (w_down.at[0], wd),
                (seq_ids, ids),
                (msg_left.at[0], ml),
                (msg_right.at[0], mr),
                (count_left, cl),
                (count_right, cr),
            )
        )
    ]
    for load in loads:
        load.start()

    greeted = 1 + has_left.astype(jnp.int32) + has_right.astype(jnp.int32)
    greeted += (on_right | on_left).astype(jnp.int32)
    greeted += RELAYS * ((me == edge_l) | (me == edge_r)).astype(jnp.int32)
    pl.semaphore_wait(barrier, greeted)

    ids_copy = remote(seq_ids, ids_p, y_send.at[0], y_recv.at[0], partner)
    tok_copy = remote(tokens.at[0], tok_p, y_send.at[1], y_recv.at[1], partner)
    wd_copies = [
        remote(
            w_down.at[0, pl.ds(r0, r)], wd_p.at[pl.ds(r0, r)], wd_send.at[c], wd_recv.at[c], partner
        )
        for c, (r0, r) in enumerate(CHUNKS)
    ]
    gh_copies = [
        remote(gh_out.at[pl.ds(r0, r)], gh_p.at[pl.ds(r0, r)], gh_send.at[c], gh_recv.at[c], partner)
        for c, (r0, r) in enumerate(CHUNKS)
    ]
    r_copies = [
        remote(
            send_r.at[:, pl.ds(r0, r)], recv_l.at[:, pl.ds(r0, r)], r_send.at[c], r_recv.at[c], right
        )
        for c, (r0, r) in enumerate(CHUNKS)
    ] + [remote(cnt_r_out, cnt_l, r_send.at[n], r_recv.at[n], right)]
    l_copies = [
        remote(
            send_l.at[:, pl.ds(r0, r)], recv_r.at[:, pl.ds(r0, r)], l_send.at[c], l_recv.at[c], left
        )
        for c, (r0, r) in enumerate(CHUNKS)
    ] + [remote(cnt_l_out, cnt_r, l_send.at[n], l_recv.at[n], left)]
    to_left = remote(
        relay_buf, recv_l.at[piece % 2, piece_rows], relay_send, r_recv.at[piece_chunk], (edge_l, side)
    )
    to_right = remote(
        relay_buf, recv_r.at[piece % 2, piece_rows], relay_send, l_recv.at[piece_chunk], (edge_r, side)
    )

    arrival = remote(relay_buf, relay_buf, relay_send, relay_recv, (edge_l, side))

    def send_pieces(c, source, send, relay):
        r0, r = CHUNKS[c]
        for p in range(r0 // PIECE * 2, (r0 + r) // PIECE * 2):
            remote(
                source.at[p % 2, pl.ds(p // 2 * PIECE, PIECE)], relay_buf, send.at[c], relay_recv, relay(p)
            ).start()

    def send_chain(c):
        @pl.when((has_right & (me != edge_r)) if relayed[c] else has_right)
        def _():
            r_copies[c].start()

        @pl.when((has_left & (me != edge_l)) if relayed[c] else has_left)
        def _():
            l_copies[c].start()

        if relayed[c]:

            @pl.when(me == edge_r)
            def _():
                send_pieces(c, send_r, r_send, relay_right)

            @pl.when(me == edge_l)
            def _():
                send_pieces(c, send_l, l_send, relay_left)

    def forward(c):
        if c >= 0 and relayed[c]:

            @pl.when(on_right & (piece_chunk == c))
            def _():
                arrival.wait_recv()
                to_left.start()

            @pl.when(on_left & (piece_chunk == c))
            def _():
                arrival.wait_recv()
                to_right.start()

    ids_copy.start()
    wd_copies[0].start()
    tok_copy.start()

    @pl.when(jnp.logical_not(has_left))
    def _():
        recv_l[...] = jnp.zeros_like(recv_l)
        cnt_l[...] = jnp.zeros_like(cnt_l)

    @pl.when(jnp.logical_not(has_right))
    def _():
        recv_r[...] = jnp.zeros_like(recv_r)
        cnt_r[...] = jnp.zeros_like(cnt_r)

    loads[0].wait()
    loads[1].wait()
    w_all = wp[...].reshape(2 * hidden, width)
    gate_own, up_own = gate_factors(dot_nt(w_all, tok[...]) * width_scale, hidden)

    loads[4].wait()
    ids_copy.wait_recv()
    own_row = ids[...]
    shape = (rows, rows)
    diag = lax.broadcasted_iota(jnp.int32, shape, 0) == lax.broadcasted_iota(jnp.int32, shape, 1)
    own_col = jnp.sum(jnp.where(diag, own_row, 0), axis=1, keepdims=True)
    peer_col = jnp.sum(jnp.where(diag, ids_p[...], 0), axis=1, keepdims=True)
    seq_len = jnp.sum((own_col == own_row).astype(F32), axis=0, keepdims=True) + jnp.sum(
        (peer_col == own_row).astype(F32), axis=0, keepdims=True
    )
    weight[...] = (2 * rows / SEQS) / seq_len * width_scale

    loads[2].wait()
    loads[3].wait()
    gh_own = dot_nt(wd[...], cot[...]) * weight[...]
    lhs[:hidden] = (gh_own * gate_own).astype(BF16)
    lhs[hidden:] = (gh_own * up_own).astype(BF16)

    def own_tile(j, carry):
        part = jnp.dot(lhs[...], tok[:, cols(j)], preferred_element_type=F32)
        part = part.reshape(2, hidden, TILE) * (learn_rate * batch_scale)
        half[:, :, cols(j)] = wp[:, :, cols(j)].astype(F32) - part
        return carry

    lax.fori_loop(0, tiles, own_tile, 0)

    def partner_grad_hidden(c):
        r0, r = CHUNKS[c]
        wd_copies[c].wait_recv()
        gh = dot_nt(wd_p[r0 : r0 + r], cot[...]) * weight[...]
        gh_out[r0 : r0 + r] = gh.astype(BF16)
        gh_copies[c].start()

    def finish_rows(c):
        r0, r = CHUNKS[c]
        gh_copies[c].wait_recv()
        gh = gh_p[r0 : r0 + r].astype(F32)
        both = jnp.concatenate(
            [gh * fac_gate[r0 : r0 + r], gh * fac_up[r0 : r0 + r]], axis=0
        ).astype(BF16)

        def tile(j, carry):
            part = jnp.dot(both, tok_p[:, cols(j)], preferred_element_type=F32)
            part = part.reshape(2, r, TILE) * (learn_rate * batch_scale)
            step = half[:, r0 : r0 + r, cols(j)] - part
            half[:, r0 : r0 + r, cols(j)] = step
            send_r[:, r0 : r0 + r, cols(j)] = (
                step + ml[:, r0 : r0 + r, cols(j)].astype(F32)
            ).astype(BF16)
            send_l[:, r0 : r0 + r, cols(j)] = (
                step + mr[:, r0 : r0 + r, cols(j)].astype(F32)
            ).astype(BF16)
            return carry

        lax.fori_loop(0, tiles, tile, 0)
        send_chain(c)
        forward(c - 1)

    partner_grad_hidden(0)
    for c in range(1, min(3, n)):
        wd_copies[c].start()

    for k in (5, 6, 7, 8):
        loads[k].wait()
    cnt_r_out[...] = jnp.full(cnt_r_out.shape, 1 + cl[0], jnp.int32)
    cnt_l_out[...] = jnp.full(cnt_l_out.shape, 1 + cr[0], jnp.int32)
    send_chain(n)

    tok_copy.wait_recv()
    gate_peer, up_peer = gate_factors(dot_nt(w_all, tok_p[...]) * width_scale, hidden)
    fac_gate[...] = gate_peer
    fac_up[...] = up_peer
    finish_rows(0)
    for c in range(1, n):
        partner_grad_hidden(c)
        if c + 2 < n:
            wd_copies[c + 2].start()
        if c >= 2:
            finish_rows(c - 1)
    finish_rows(n - 1)

    @pl.when(has_left)
    def _():
        r_copies[n].wait_recv()

    @pl.when(has_right)
    def _():
        l_copies[n].wait_recv()

    inverse = 1.0 / (1.0 + cnt_l[...].astype(F32) + cnt_r[...].astype(F32))

    for c, (r0, r) in enumerate(CHUNKS):

        @pl.when(has_left)
        def _(c=c):
            r_copies[c].wait_recv()

        @pl.when(has_right)
        def _(c=c):
            l_copies[c].wait_recv()

        def tile(j, carry, r0=r0, r=r):
            total = (
                half[:, r0 : r0 + r, cols(j)]
                + recv_l[:, r0 : r0 + r, cols(j)].astype(F32)
                + recv_r[:, r0 : r0 + r, cols(j)].astype(F32)
            )
            out[0, :, r0 : r0 + r, cols(j)] = (total * inverse.reshape(1, 1, TILE)).astype(BF16)
            return carry

        lax.fori_loop(0, tiles, tile, 0)

    ids_copy.wait_send()
    tok_copy.wait_send()
    for c in range(n):
        wd_copies[c].wait_send()
        gh_copies[c].wait_send()
    for c in range(n + 1):

        @pl.when(has_right)
        def _(c=c):
            r_copies[c].wait_send()

        @pl.when(has_left)
        def _(c=c):
            l_copies[c].wait_send()

    @pl.when(on_right)
    def _():
        to_left.wait_send()

    @pl.when(on_left)
    def _():
        to_right.wait_send()


def body(w_pair, w_down, tokens, cotangent, seq_ids, msg_left, msg_right, count_left, count_right):
    workers = lax.axis_size("chain")
    pair = w_pair.shape[1:]
    hidden, width = pair[1:]
    rows = tokens.shape[1]
    n = len(CHUNKS)
    any_space = pl.BlockSpec(memory_space=pltpu.HBM)
    vm, dma = pltpu.VMEM, pltpu.SemaphoreType.DMA
    return pl.pallas_call(
        functools.partial(kernel, workers),
        out_shape=pltpu.VMEM(w_pair.shape, BF16),
        in_specs=[any_space] * 9,
        out_specs=pl.BlockSpec(memory_space=pltpu.VMEM),
        scratch_shapes=[
            vm(pair, BF16),
            vm((hidden, width), BF16),
            vm((rows, width), BF16),
            vm((rows, width), BF16),
            vm((1, rows), jnp.int32),
            vm(pair, BF16),
            vm(pair, BF16),
            pltpu.SMEM((1,), jnp.int32),
            pltpu.SMEM((1,), jnp.int32),
            vm((rows, width), BF16),
            vm((hidden, width), BF16),
            vm((1, rows), jnp.int32),
            vm((hidden, rows), BF16),
            vm((hidden, rows), BF16),
            vm((hidden, rows), F32),
            vm((hidden, rows), F32),
            vm((2 * hidden, rows), BF16),
            vm((1, rows), F32),
            vm(pair, F32),
            vm(pair, BF16),
            vm(pair, BF16),
            vm(pair, BF16),
            vm(pair, BF16),
            vm((1, TILE), jnp.int32),
            vm((1, TILE), jnp.int32),
            vm((1, TILE), jnp.int32),
            vm((1, TILE), jnp.int32),
            dma((9,)),
            dma((2,)),
            dma((2,)),
            dma((n,)),
            dma((n,)),
            dma((n,)),
            dma((n,)),
            dma((n + 1,)),
            dma((n + 1,)),
            dma((n + 1,)),
            dma((n + 1,)),
            vm((PIECE, width), BF16),
            dma(()),
            dma(()),
        ],
        compiler_params=pltpu.CompilerParams(
            collective_id=0, has_side_effects=True, vmem_limit_bytes=61 * 1024 * 1024
        ),
    )(w_pair, w_down, tokens, cotangent, seq_ids, msg_left, msg_right, count_left, count_right)


def solution(mesh):
    return jax.shard_map(
        body,
        mesh=mesh,
        in_specs=(
            P("chain", None, "shard", None),
            P("chain", "shard", None),
            P("chain", "shard", None),
            P("chain", "shard", None),
            P("chain", "shard"),
            P("chain", None, "shard", None),
            P("chain", None, "shard", None),
            P("chain"),
            P("chain"),
        ),
        out_specs=P("chain", None, "shard", None),
        check_vma=False,
    )
```

```python
import functools

import jax
import jax.numpy as jnp
from jax import lax
from jax.experimental import pallas as pl
from jax.experimental.pallas import tpu as pltpu
from jax.sharding import PartitionSpec as P

MESH = pl.DeviceIdType.MESH
F32 = jnp.float32
BF16 = jnp.bfloat16
learn_rate = 1.0
SEQS = 8

CHUNKS = tuple((r, 16) for r in range(0, 128, 16))
TILE = 1024

PIECE, CUTS = 16, 4
RELAYS = 24


def dot_nt(a, b):
    return lax.dot_general(a, b, (((1,), (1,)), ((), ())), preferred_element_type=F32)


def gate_factors(pre, hidden):
    gate, up = pre[:hidden], pre[hidden:]
    sig = jax.nn.sigmoid(gate)
    return up * sig * (1.0 + gate * (1.0 - sig)), gate * sig


def kernel(
    workers,
    w_pair,
    w_down,
    tokens,
    cotangent,
    seq_ids,
    msg_left,
    msg_right,
    count_left,
    count_right,
    out,
    wp,
    wd,
    tok,
    cot,
    ids,
    ml,
    mr,
    cl,
    cr,
    tok_p,
    wd_p,
    ids_p,
    gh_out,
    gh_p,
    fac_gate,
    fac_up,
    lhs,
    weight,
    half,
    send_r,
    send_l,
    recv_l,
    recv_r,
    cnt_r_out,
    cnt_l_out,
    cnt_l,
    cnt_r,
    load_sem,
    y_send,
    y_recv,
    wd_send,
    wd_recv,
    gh_send,
    gh_recv,
    r_send,
    r_recv,
    l_send,
    l_recv,
    relay_buf,
    relay_send,
    relay_recv,
):
    me, side = lax.axis_index("chain"), lax.axis_index("shard")
    partner = (me, 1 - side)
    last = workers - 1
    right, left = ((me + 1) % workers, side), ((me + last) % workers, side)
    has_left, has_right = me > 0, me < last
    rows, width = tok.shape
    hidden = wd.shape[0]
    width_scale = width**-0.5
    batch_scale = (2 * rows) ** -0.5
    n = len(CHUNKS)
    tiles = width // TILE

    def remote(src, dst, send, recv, device):
        return pltpu.make_async_remote_copy(
            src_ref=src, dst_ref=dst, send_sem=send, recv_sem=recv, device_id=device, device_id_type=MESH
        )

    def cols(j):
        return pl.ds(pl.multiple_of(j * TILE, TILE), TILE)

    core, upper = me % 2, me >= workers // 2
    column = jnp.where(upper, last - me, me) // 2
    is_edge = column == 0
    is_relay = (column >= 1) & (column <= RELAYS)
    edge = jnp.where(upper, last - 1 + core, core)
    piece = jnp.where(is_relay, column - 1, 0)

    def relay(p):
        return jnp.where(upper, edge - 2 * (p + 1), edge + 2 * (p + 1))

    def piece_of(p):
        first, start = p // CUTS * PIECE, p % CUTS * (width // CUTS)
        if not isinstance(p, int):
            first, start = pl.multiple_of(first, PIECE), pl.multiple_of(start, width // CUTS)
        return pl.ds(first, PIECE), pl.ds(start, width // CUTS)

    barrier = pltpu.get_barrier_semaphore()
    pl.semaphore_signal(barrier, inc=1, device_id=partner, device_id_type=MESH)

    @pl.when(has_left)
    def _():
        pl.semaphore_signal(barrier, inc=1, device_id=left, device_id_type=MESH)

    @pl.when(has_right)
    def _():
        pl.semaphore_signal(barrier, inc=1, device_id=right, device_id_type=MESH)

    @pl.when(is_relay)
    def _():
        pl.semaphore_signal(barrier, inc=1, device_id=(edge, 1 - side), device_id_type=MESH)

    loads = [
        pltpu.make_async_copy(src, dst, load_sem.at[k])
        for k, (src, dst) in enumerate(
            (
                (tokens.at[0], tok),
                (w_pair.at[0], wp),
                (cotangent.at[0], cot),
                (w_down.at[0], wd),
                (seq_ids, ids),
                (msg_left.at[0], ml),
                (msg_right.at[0], mr),
                (count_left, cl),
                (count_right, cr),
            )
        )
    ]
    for load in loads:
        load.start()

    greeted = 1 + has_left.astype(jnp.int32) + has_right.astype(jnp.int32)
    greeted += RELAYS * is_edge.astype(jnp.int32)
    pl.semaphore_wait(barrier, greeted)

    ids_copy = remote(seq_ids, ids_p, y_send.at[0], y_recv.at[0], partner)
    tok_copy = remote(tokens.at[0], tok_p, y_send.at[1], y_recv.at[1], partner)
    wd_copies = [
        remote(
            w_down.at[0, pl.ds(r0, r)], wd_p.at[pl.ds(r0, r)], wd_send.at[c], wd_recv.at[c], partner
        )
        for c, (r0, r) in enumerate(CHUNKS)
    ]
    gh_copies = [
        remote(gh_out.at[pl.ds(r0, r)], gh_p.at[pl.ds(r0, r)], gh_send.at[c], gh_recv.at[c], partner)
        for c, (r0, r) in enumerate(CHUNKS)
    ]
    r_copies = [
        remote(
            send_r.at[:, pl.ds(r0, r)], recv_l.at[:, pl.ds(r0, r)], r_send.at[c], r_recv.at[c], right
        )
        for c, (r0, r) in enumerate(CHUNKS)
    ] + [remote(cnt_r_out, cnt_l, r_send.at[n], r_recv.at[n], right)]
    l_copies = [
        remote(
            send_l.at[:, pl.ds(r0, r)], recv_r.at[:, pl.ds(r0, r)], l_send.at[c], l_recv.at[c], left
        )
        for c, (r0, r) in enumerate(CHUNKS)
    ] + [remote(cnt_l_out, cnt_r, l_send.at[n], l_recv.at[n], left)]
    taken = RELAYS // CUTS * PIECE
    rest = pl.ds(taken, rows - taken)
    rest_copy = remote(tokens.at[0, rest], tok_p.at[rest], y_send.at[1], y_recv.at[1], partner)
    handed = remote(relay_buf, tok_p.at[piece_of(piece)], relay_send, y_recv.at[1], (edge, side))

    def send_chain(c):
        @pl.when(has_right)
        def _():
            r_copies[c].start()

        @pl.when(has_left)
        def _():
            l_copies[c].start()

    ids_copy.start()
    wd_copies[0].start()

    @pl.when(jnp.logical_not(is_edge))
    def _():
        tok_copy.start()

    @pl.when(is_edge)
    def _():
        rest_copy.start()
        for p in range(RELAYS):
            at = piece_of(p)
            remote(
                tokens.at[(0, *at)], relay_buf, y_send.at[1], relay_recv, (relay(p), 1 - side)
            ).start()

    @pl.when(jnp.logical_not(has_left))
    def _():
        recv_l[...] = jnp.zeros_like(recv_l)
        cnt_l[...] = jnp.zeros_like(cnt_l)

    @pl.when(jnp.logical_not(has_right))
    def _():
        recv_r[...] = jnp.zeros_like(recv_r)
        cnt_r[...] = jnp.zeros_like(cnt_r)

    loads[0].wait()
    loads[1].wait()
    w_all = wp[...].reshape(2 * hidden, width)
    gate_own, up_own = gate_factors(dot_nt(w_all, tok[...]) * width_scale, hidden)

    loads[4].wait()
    ids_copy.wait_recv()
    own_row = ids[...]
    shape = (rows, rows)
    diag = lax.broadcasted_iota(jnp.int32, shape, 0) == lax.broadcasted_iota(jnp.int32, shape, 1)
    own_col = jnp.sum(jnp.where(diag, own_row, 0), axis=1, keepdims=True)
    peer_col = jnp.sum(jnp.where(diag, ids_p[...], 0), axis=1, keepdims=True)
    seq_len = jnp.sum((own_col == own_row).astype(F32), axis=0, keepdims=True) + jnp.sum(
        (peer_col == own_row).astype(F32), axis=0, keepdims=True
    )
    weight[...] = (2 * rows / SEQS) / seq_len * width_scale

    loads[2].wait()
    loads[3].wait()
    gh_own = dot_nt(wd[...], cot[...]) * weight[...]
    lhs[:hidden] = (gh_own * gate_own).astype(BF16)
    lhs[hidden:] = (gh_own * up_own).astype(BF16)

    def own_tile(j, carry):
        part = jnp.dot(lhs[...], tok[:, cols(j)], preferred_element_type=F32)
        part = part.reshape(2, hidden, TILE) * (learn_rate * batch_scale)
        half[:, :, cols(j)] = wp[:, :, cols(j)].astype(F32) - part
        return carry

    lax.fori_loop(0, tiles, own_tile, 0)

    def partner_grad_hidden(c):
        r0, r = CHUNKS[c]
        wd_copies[c].wait_recv()
        gh = dot_nt(wd_p[r0 : r0 + r], cot[...]) * weight[...]
        gh_out[r0 : r0 + r] = gh.astype(BF16)
        gh_copies[c].start()

    def finish_rows(c):
        r0, r = CHUNKS[c]
        gh_copies[c].wait_recv()
        gh = gh_p[r0 : r0 + r].astype(F32)
        both = jnp.concatenate(
            [gh * fac_gate[r0 : r0 + r], gh * fac_up[r0 : r0 + r]], axis=0
        ).astype(BF16)

        def tile(j, carry):
            part = jnp.dot(both, tok_p[:, cols(j)], preferred_element_type=F32)
            part = part.reshape(2, r, TILE) * (learn_rate * batch_scale)
            step = half[:, r0 : r0 + r, cols(j)] - part
            half[:, r0 : r0 + r, cols(j)] = step
            send_r[:, r0 : r0 + r, cols(j)] = (
                step + ml[:, r0 : r0 + r, cols(j)].astype(F32)
            ).astype(BF16)
            send_l[:, r0 : r0 + r, cols(j)] = (
                step + mr[:, r0 : r0 + r, cols(j)].astype(F32)
            ).astype(BF16)
            return carry

        lax.fori_loop(0, tiles, tile, 0)
        send_chain(c)

    partner_grad_hidden(0)

    @pl.when(is_relay)
    def _():
        remote(relay_buf, relay_buf, relay_send, relay_recv, (edge, side)).wait_recv()
        handed.start()

    for c in range(1, min(3, n)):
        wd_copies[c].start()

    for k in (5, 6, 7, 8):
        loads[k].wait()
    cnt_r_out[...] = jnp.full(cnt_r_out.shape, 1 + cl[0], jnp.int32)
    cnt_l_out[...] = jnp.full(cnt_l_out.shape, 1 + cr[0], jnp.int32)
    send_chain(n)

    tok_copy.wait_recv()
    gate_peer, up_peer = gate_factors(dot_nt(w_all, tok_p[...]) * width_scale, hidden)
    fac_gate[...] = gate_peer
    fac_up[...] = up_peer
    finish_rows(0)
    for c in range(1, n):
        partner_grad_hidden(c)
        if c + 2 < n:
            wd_copies[c + 2].start()
        if c >= 2:
            finish_rows(c - 1)
    finish_rows(n - 1)

    @pl.when(has_left)
    def _():
        r_copies[n].wait_recv()

    @pl.when(has_right)
    def _():
        l_copies[n].wait_recv()

    inverse = 1.0 / (1.0 + cnt_l[...].astype(F32) + cnt_r[...].astype(F32))

    for c, (r0, r) in enumerate(CHUNKS):

        @pl.when(has_left)
        def _(c=c):
            r_copies[c].wait_recv()

        @pl.when(has_right)
        def _(c=c):
            l_copies[c].wait_recv()

        def tile(j, carry, r0=r0, r=r):
            total = (
                half[:, r0 : r0 + r, cols(j)]
                + recv_l[:, r0 : r0 + r, cols(j)].astype(F32)
                + recv_r[:, r0 : r0 + r, cols(j)].astype(F32)
            )
            out[0, :, r0 : r0 + r, cols(j)] = (total * inverse.reshape(1, 1, TILE)).astype(BF16)
            return carry

        lax.fori_loop(0, tiles, tile, 0)

    ids_copy.wait_send()
    tok_copy.wait_send()
    for c in range(n):
        wd_copies[c].wait_send()
        gh_copies[c].wait_send()
    for c in range(n + 1):

        @pl.when(has_right)
        def _(c=c):
            r_copies[c].wait_send()

        @pl.when(has_left)
        def _(c=c):
            l_copies[c].wait_send()

    @pl.when(is_relay)
    def _():
        handed.wait_send()


def body(w_pair, w_down, tokens, cotangent, seq_ids, msg_left, msg_right, count_left, count_right):
    workers = lax.axis_size("chain")
    pair = w_pair.shape[1:]
    hidden, width = pair[1:]
    rows = tokens.shape[1]
    n = len(CHUNKS)
    any_space = pl.BlockSpec(memory_space=pltpu.HBM)
    vm, dma = pltpu.VMEM, pltpu.SemaphoreType.DMA
    return pl.pallas_call(
        functools.partial(kernel, workers),
        out_shape=pltpu.VMEM(w_pair.shape, BF16),
        in_specs=[any_space] * 9,
        out_specs=pl.BlockSpec(memory_space=pltpu.VMEM),
        scratch_shapes=[
            vm(pair, BF16),
            vm((hidden, width), BF16),
            vm((rows, width), BF16),
            vm((rows, width), BF16),
            vm((1, rows), jnp.int32),
            vm(pair, BF16),
            vm(pair, BF16),
            pltpu.SMEM((1,), jnp.int32),
            pltpu.SMEM((1,), jnp.int32),
            vm((rows, width), BF16),
            vm((hidden, width), BF16),
            vm((1, rows), jnp.int32),
            vm((hidden, rows), BF16),
            vm((hidden, rows), BF16),
            vm((hidden, rows), F32),
            vm((hidden, rows), F32),
            vm((2 * hidden, rows), BF16),
            vm((1, rows), F32),
            vm(pair, F32),
            vm(pair, BF16),
            vm(pair, BF16),
            vm(pair, BF16),
            vm(pair, BF16),
            vm((1, TILE), jnp.int32),
            vm((1, TILE), jnp.int32),
            vm((1, TILE), jnp.int32),
            vm((1, TILE), jnp.int32),
            dma((9,)),
            dma((2,)),
            dma((2,)),
            dma((n,)),
            dma((n,)),
            dma((n,)),
            dma((n,)),
            dma((n + 1,)),
            dma((n + 1,)),
            dma((n + 1,)),
            dma((n + 1,)),
            vm((PIECE, width // CUTS), BF16),
            dma(()),
            dma(()),
        ],
        compiler_params=pltpu.CompilerParams(
            collective_id=0, has_side_effects=True, vmem_limit_bytes=61 * 1024 * 1024
        ),
    )(w_pair, w_down, tokens, cotangent, seq_ids, msg_left, msg_right, count_left, count_right)


def solution(mesh):
    return jax.shard_map(
        body,
        mesh=mesh,
        in_specs=(
            P("chain", None, "shard", None),
            P("chain", "shard", None),
            P("chain", "shard", None),
            P("chain", "shard", None),
            P("chain", "shard"),
            P("chain", None, "shard", None),
            P("chain", None, "shard", None),
            P("chain"),
            P("chain"),
        ),
        out_specs=P("chain", None, "shard", None),
        check_vma=False,
    )
```
